32 devices in a mesh: samples: 4 (over y, x), features: 4 (over z), rhs: 2 (over core).
Axes of the slice: x: 2, y: 2, z: 4, core: 2. Of those that a mesh axis runs over, the one named last changes fastest.
Arguments:
- design: bfloat16 [32768, 32768], P(('samples', 'rhs'), 'features'), may hold values from -0.03125 to 0.03125
- right_side: float32 [32768, 64], P('features', 'rhs'), may hold values from -6 to 6
- factor: bfloat16 [32768, 768], P('features', 'rhs'), may hold values from -0.03125 to 0.03125
- nystrom_values: float32 [768], replicated, may hold values from 0.5 to 3
Outputs:
- solution: float32 [32768, 64], P('features', 'rhs')
- residual: float32 [32768, 64], P('features', 'rhs')
The draws below stay inside these ranges and needn't reach their ends.
All inputs are finite; a program needn't handle non-finite values.
Results may differ from the reference program's by a relative error of at most 0.0181.
Values may be sent and summed in bfloat16 or wider, within the bound.
A program may use at most 192 MiB of HBM per device.

```python
import math
import jax
import jax.numpy as jnp
from jax import lax

F = 32768
K = 64
R = 768
ITERS = 3
NS = 32768


def block_levels(key, shape, cuts, low, top_value):
    level, own = 1.0, jax.random.fold_in(key, 6)
    for dim, shards_of in cuts:
        steps = jnp.exp(jax.random.uniform(jax.random.fold_in(own, dim), (shards_of,), jnp.float32, low / len(cuts), top_value / len(cuts)))
        level = level * jnp.repeat(steps, shape[dim] // shards_of).reshape([-1 if axis == dim else 1 for axis in range(len(shape))])
    return level


def scatter_about(rng, extent, deviation, most, pieces=(), held_as=jnp.bfloat16):
    factor_of = block_levels(rng, extent, pieces, -0.22, 0.18) if pieces else 1.0
    array = jax.random.normal(rng, extent, jnp.float32) * deviation * factor_of
    return jnp.minimum(jnp.maximum(array, -most), most).astype(held_as)


def setup_inputs(seed: int = 0) -> dict:
    splits = jax.random.split(jax.random.key(seed), 5)
    design = scatter_about(splits[0], (NS, F), NS ** -0.5, 0.03125, ((0, 8), (1, 4)))
    right_side = scatter_about(splits[1], (F, K), 1.0, 6.0, ((0, 4), (1, 2)), jnp.float32)
    factor = scatter_about(splits[2], (F, R), F ** -0.5, 0.03125, ((0, 4), (1, 2)))
    nystrom_values = jnp.clip(jnp.exp(jax.random.uniform(splits[3], (R,), jnp.float32, math.log(0.5), math.log(3.0))), 0.5, 3.0)
    return {"design": design, "right_side": right_side, "factor": factor, "nystrom_values": nystrom_values}


ridge_weight = 1.0

def inner_prod(left, right):
    return lax.dot_general(left.astype(jnp.float32), right.astype(jnp.float32), (((0,), (0,)), ((), ())), precision=lax.Precision.HIGHEST, preferred_element_type=jnp.float32)

def apply_operator(design, direction):
    narrow = direction.astype(jnp.bfloat16)
    images = jnp.dot(design.astype(jnp.float32), narrow.astype(jnp.float32), preferred_element_type=jnp.float32).astype(jnp.bfloat16)
    summed = lax.dot_general(design.astype(jnp.float32), images.astype(jnp.float32), (((0,), (0,)), ((), ())), preferred_element_type=jnp.float32)
    return summed + ridge_weight * direction

def reference(design, right_side, factor, nystrom_values):
    shrink = (1.0 + jnp.min(nystrom_values)) / (1.0 + nystrom_values) - 1.0
    factor_wide = factor.astype(jnp.float32)

    def precondition(values):
        projected = inner_prod(factor_wide, values)
        return values + jnp.dot(factor_wide, shrink[:, None] * projected, precision=lax.Precision.HIGHEST)
    solution = jnp.zeros_like(right_side)
    residual = right_side
    direction = precondition(residual)
    for iteration in range(ITERS):
        applied = apply_operator(design, direction)
        gram_block = inner_prod(direction, applied)
        gram_block = 0.5 * (gram_block + gram_block.T)
        chol_lower = jnp.linalg.cholesky(gram_block)
        unit_dir = jax.scipy.linalg.solve_triangular(chol_lower, direction.T, lower=True).T
        unit_img = jax.scipy.linalg.solve_triangular(chol_lower, applied.T, lower=True).T
        step_coef = jax.scipy.linalg.solve_triangular(chol_lower, inner_prod(direction, residual), lower=True)
        solution = solution + jnp.dot(unit_dir, step_coef, precision=lax.Precision.HIGHEST)
        residual = residual - jnp.dot(unit_img, step_coef, precision=lax.Precision.HIGHEST)
        if iteration + 1 < ITERS:
            scaled = precondition(residual)
            next_coef = -inner_prod(unit_img, scaled)
            direction = scaled + jnp.dot(unit_dir, next_coef, precision=lax.Precision.HIGHEST)
    return (solution, residual)
```

```python
import functools

import jax
import jax.numpy as jnp
from jax import lax
from jax.experimental import pallas as pl
from jax.experimental.pallas import tpu as pltpu
from jax.sharding import PartitionSpec as P

ITERS = 3
MESH = pl.DeviceIdType.MESH
RIDGE = 1.0


def dot_t(left, right):
    return lax.dot_general(
        left,
        right,
        (((1,), (1,)), ((), ())),
        precision=lax.Precision.HIGHEST,
        preferred_element_type=jnp.float32,
    )


def dot_h(left, right):
    return jnp.dot(
        left, right, precision=lax.Precision.HIGHEST, preferred_element_type=jnp.float32
    )


def feature_group(n_rhs):
    me = lax.axis_index("samples") * n_rhs + lax.axis_index("rhs")

    def place(index):
        return {"samples": lax.div(index, n_rhs), "rhs": lax.rem(index, n_rhs)}

    return me, place


def sample_group():
    return lax.axis_index("features"), lambda index: {"features": index}


def others(n, me, body):
    for step in range(1, n):
        body(lax.rem(me + step, n))


def greet(groups):
    barrier = pltpu.get_barrier_semaphore()
    total = 0
    for n, me, place in groups:
        others(
            n,
            me,
            lambda peer: pl.semaphore_signal(
                barrier, inc=1, device_id=place(peer), device_id_type=MESH
            ),
        )
        total += n - 1
    pl.semaphore_wait(barrier, total)


def columns(index, width):
    return pl.ds(pl.multiple_of(index * width, 128), width)


def exchange(n, me, place, source, target, send_sem, recv_sem):
    def copy(step):
        peer = lax.rem(me + step, n)
        return pltpu.make_async_remote_copy(
            src_ref=source(peer),
            dst_ref=target(me),
            send_sem=send_sem.at[step],
            recv_sem=recv_sem.at[step],
            device_id=place(peer),
            device_id_type=MESH,
        )

    copies = [copy(step) for step in range(1, n)]
    for each in copies:
        each.start()
    for each in copies:
        each.wait_recv()
    return copies


def finish(copies):
    for each in copies:
        each.wait_send()


def total_of(own, held, n, me):
    total = own.astype(jnp.float32)
    for step in range(1, n):
        total = total + held[lax.rem(me + step, n)].astype(jnp.float32)
    return total


def images_kernel(n, x_ref, out_ref, held, send_a, recv_a, send_b, recv_b):
    me, place = sample_group()
    width = x_ref.shape[1] // n
    greet([(n, me, place)])
    first = exchange(
        n, me, place,
        lambda peer: x_ref.at[:, columns(peer, width)],
        lambda index: held.at[index],
        send_a, recv_a,
    )
    own = x_ref[:, columns(me, width)]
    out_ref[:, columns(me, width)] = total_of(own, held, n, me).astype(out_ref.dtype)
    second = exchange(
        n, me, place,
        lambda peer: out_ref.at[:, columns(me, width)],
        lambda index: out_ref.at[:, columns(index, width)],
        send_b, recv_b,
    )
    finish(first + second)


def scatter_kernel(n, n_rhs, x_ref, out_ref, held, send_a, recv_a):
    me, place = feature_group(n_rhs)
    width = x_ref.shape[1] // n
    greet([(n, me, place)])
    first = exchange(
        n, me, place,
        lambda peer: x_ref.at[:, columns(peer, width)],
        lambda index: held.at[index],
        send_a, recv_a,
    )
    out_ref[...] = total_of(x_ref[:, columns(me, width)], held, n, me)
    finish(first)


def gather_kernel(n, n_rhs, split, x_ref, out_ref, send_a, recv_a):
    me, place = feature_group(n_rhs)
    rows, wide = out_ref.shape
    width = wide // n

    def part(peer):
        if split:
            return pl.ds(pl.multiple_of(lax.rem(peer, n_rhs) * rows, 16), rows)
        return pl.ds(0, rows)

    greet([(n, me, place)])
    first = exchange(
        n, me, place,
        lambda peer: x_ref.at[part(peer), :],
        lambda index: out_ref.at[:, columns(index, width)],
        send_a, recv_a,
    )
    out_ref[:, columns(me, width)] = x_ref[part(me), :]
    finish(first)


def totals_kernel(
    n, n_rhs, n_feat, x_ref, out_ref, held, across, mine, sa, ra, sb, rb, sc, rc
):
    me, place = feature_group(n_rhs)
    feat, feat_place = sample_group()
    width = x_ref.shape[1] // n
    greet([(n, me, place), (n_feat, feat, feat_place)])
    first = exchange(
        n, me, place,
        lambda peer: x_ref.at[:, columns(peer, width)],
        lambda index: held.at[index],
        sa, ra,
    )
    mine[...] = total_of(x_ref[:, columns(me, width)], held, n, me)
    second = exchange(
        n_feat, feat, feat_place,
        lambda peer: mine,
        lambda index: across.at[index],
        sb, rb,
    )
    across[feat] = mine[...]
    total = across[0]
    for index in range(1, n_feat):
        total = total + across[index]
    out_ref[:, columns(me, width)] = total
    third = exchange(
        n, me, place,
        lambda peer: out_ref.at[:, columns(me, width)],
        lambda index: out_ref.at[:, columns(index, width)],
        sc, rc,
    )
    finish(first + second + third)


def call(kernel, name, ident, shape, dtype, scratch, sems, *args):
    return pl.pallas_call(
        kernel,
        name=name,
        out_shape=jax.ShapeDtypeStruct(shape, dtype),
        in_specs=[pl.BlockSpec(memory_space=pltpu.VMEM)] * len(args),
        out_specs=pl.BlockSpec(memory_space=pltpu.VMEM),
        scratch_shapes=[pltpu.VMEM(s, d) for s, d in scratch]
        + [pltpu.SemaphoreType.DMA((count,)) for count in sems],
        compiler_params=pltpu.CompilerParams(collective_id=ident, has_side_effects=True),
    )(*args)


def shards(n_samp, n_feat, n_rhs, design, right_side, factor, nystrom_values):
    feat_rows, col_share = right_side.shape
    samples = design.shape[0]
    width = col_share * n_rhs
    rank = nystrom_values.shape[0]
    n = n_samp * n_rhs
    piece = feat_rows // n
    samp, rhs = lax.axis_index("samples"), lax.axis_index("rhs")
    shrink = (1.0 + jnp.min(nystrom_values)) / (1.0 + nystrom_values) - 1.0

    def own_rows(block):
        def rows_for(core):
            return lax.dynamic_slice_in_dim(block, (samp * n_rhs + core) * piece, piece, 0)

        parts = [None] * n_rhs
        moved = [rows_for(rhs)]
        for step in range(1, n_rhs):
            pairs = [(i, (i + step) % n_rhs) for i in range(n_rhs)]
            moved.append(lax.ppermute(rows_for((rhs + step) % n_rhs), "rhs", pairs))
        for core in range(n_rhs):
            best = moved[0]
            for step in range(1, n_rhs):
                best = jnp.where((rhs - step) % n_rhs == core, moved[step], best)
            parts[core] = best
        return jnp.concatenate(parts, axis=1)

    images_of = lambda x: call(
        functools.partial(images_kernel, n_feat), "images_sum", 1, x.shape, jnp.bfloat16,
        [((n_feat, width, samples // n_feat), jnp.bfloat16)], [n_feat] * 4, x,
    )
    scatter = lambda x: call(
        functools.partial(scatter_kernel, n, n_rhs), "feature_scatter", 2,
        (width, piece), jnp.float32, [((n, width, piece), jnp.bfloat16)], [n] * 2, x,
    )
    gather = lambda x: call(
        functools.partial(gather_kernel, n, n_rhs, False), "direction_gather", 3,
        (width, feat_rows), x.dtype, [], [n] * 2, x,
    )
    gather_out = lambda x: call(
        functools.partial(gather_kernel, n, n_rhs, True), "output_gather", 4,
        (x.shape[0] // n_rhs, feat_rows), x.dtype, [], [n] * 2, x,
    )

    def totals(x):
        lanes = x.shape[1]
        unit = 128 * n
        padded = -(-lanes // unit) * unit
        x = jnp.pad(x, ((0, 0), (0, padded - lanes)))
        share = (width, padded // n)
        got = call(
            functools.partial(totals_kernel, n, n_rhs, n_feat), "small_totals", 5,
            x.shape, jnp.float32,
            [((n,) + share, jnp.float32), ((n_feat,) + share, jnp.float32), (share, jnp.float32)],
            [n, n, n_feat, n_feat, n, n], x,
        )
        return got[:, :lanes]

    basis = own_rows(factor)
    residual = own_rows(right_side).T

    def parts_of(values):
        upper = values.astype(jnp.bfloat16)
        widened = lax.optimization_barrier(upper).astype(jnp.float32)
        return jnp.concatenate([upper, (values - widened).astype(jnp.bfloat16)], axis=0)

    def factor_inner(values):
        both = jnp.dot(parts_of(values), basis, preferred_element_type=jnp.float32)
        return both[:width] + both[width:]

    def expand(projected):
        both = lax.dot_general(
            parts_of(shrink[None, :] * projected), basis, (((1,), (1,)), ((), ())),
            preferred_element_type=jnp.float32,
        )
        return both[:width] + both[width:]

    projected = totals(factor_inner(residual))
    direction = residual + expand(projected)
    solution = jnp.zeros_like(residual)
    eye = jnp.eye(width, dtype=jnp.float32)
    for iteration in range(ITERS):
        narrow = gather(direction.astype(jnp.bfloat16))
        partial = lax.dot_general(
            narrow, design, (((1,), (1,)), ((), ())), preferred_element_type=jnp.float32
        )
        images = images_of(partial.astype(jnp.bfloat16))
        feature_term = jnp.dot(images, design, preferred_element_type=jnp.float32)
        applied = scatter(feature_term.astype(jnp.bfloat16)) + RIDGE * direction
        last = iteration + 1 == ITERS
        block = dot_t(
            jnp.concatenate([direction, applied], axis=0),
            jnp.concatenate([applied, residual], axis=0),
        )
        small = [block[:width], block[width:]]
        if not last:
            small.append(factor_inner(applied))
        summed = totals(jnp.concatenate(small, axis=1))
        gram = summed[:, :width]
        cross = summed[:, width : 2 * width]
        gram = 0.5 * (gram + gram.T)
        chol_lower = jnp.linalg.cholesky(gram)
        inverse = jax.scipy.linalg.solve_triangular(chol_lower, eye, lower=True)
        back_t = dot_h(dot_h(inverse, cross).T, inverse)
        solution = solution + dot_h(back_t, direction)
        residual = residual - dot_h(back_t, applied)
        if not last:
            image_image = summed[:, 2 * width : 3 * width]
            image_res = summed[:, 3 * width : 4 * width]
            factor_image = summed[:, 4 * width :]
            projected = projected - dot_h(back_t, factor_image)
            scaled = residual + expand(projected)
            image_new = image_res - dot_t(image_image, back_t)
            image_new = image_new + dot_t(factor_image, shrink[None, :] * projected)
            next_t = dot_h(dot_h(inverse, image_new).T, inverse)
            direction = scaled - dot_h(next_t, direction)
    stacked = []
    for core in range(n_rhs):
        rows = slice(core * col_share, (core + 1) * col_share)
        stacked += [solution[rows], residual[rows]]
    whole = gather_out(jnp.concatenate(stacked, axis=0).astype(jnp.bfloat16))
    whole = whole.astype(jnp.float32)
    return whole[:col_share].T, whole[col_share:].T


def solution(mesh):
    placed = (P(("samples", "rhs"), "features"), P("features", "rhs"), P("features", "rhs"), P())
    sizes = (mesh.shape["samples"], mesh.shape["features"], mesh.shape["rhs"])
    return jax.shard_map(
        functools.partial(shards, *sizes),
        mesh=mesh,
        in_specs=placed,
        out_specs=(P("features", "rhs"), P("features", "rhs")),
        check_vma=False,
    )
```
